32 devices in a mesh: gx: 4 (over x, core), gy: 4 (over z), gz: 2 (over y).
Axes of the slice: x: 2, y: 2, z: 4, core: 2. Of those that a mesh axis runs over, the one named last changes fastest.
Arguments:
- incidence: int32 [4, 4, 2, 2, 16, 8, 128], P('gx', 'gy', 'gz'), may hold values from 0 to 1, as said below
- live_counts: int32 [4, 4, 2, 2], P('gx', 'gy', 'gz'), may hold values from 1 to 16, as said below
- lame_first: float32 [4, 4, 2, 2, 16], P('gx', 'gy', 'gz'), may hold values from 0.5 to 2
- shear_modulus: float32 [4, 4, 2, 2, 16], P('gx', 'gy', 'gz'), may hold values from 0.5 to 4.5
- stretch: float32 [3, 4, 4, 2, 2, 16], P(None, 'gx', 'gy', 'gz'), may hold values from 0.5 to 2
Outputs:
- stiffness: float32 [4, 4, 2, 3, 128, 3, 128], P('gx', 'gy', 'gz')
The draws below stay inside these ranges and needn't reach their ends.
Inputs may be any that keep to these rules, and one draw needn't show every extreme that they name: `incidence`: each element slot names 8 distinct nodes of the tile, some corners replaced by all-zero rows; corner 0 of every slot is always present. `live_counts`: among the 2 tiles of one element block and one node block, at least one has exactly 16 live slots.
All inputs are finite; a program needn't handle non-finite values.
Results may differ from the reference program's by a relative error of at most 0.000059.
Values sent between devices are 32-bit elements; how exact they have to be, the bound alone decides.
No kernel may reach another device: no remote copies, remote signals or barrier semaphores. Data moves between devices by JAX's collectives and lax.ppermute only.
A program may use at most 64 MiB of HBM per device.

```python
import math
import jax
import jax.numpy as jnp
import numpy as np
from jax import lax

TILE = 128
CAP = 16
NTB = 2
N_GX = 4
N_GY = 4
N_GZ = 2


def draw_incidence(key, part):
    base_shape = (N_GX, N_GY, N_GZ, NTB, CAP)
    key_order = jax.random.fold_in(key, 11)
    key_keep = jax.random.fold_in(key, 12)
    scores = jax.random.randint(key_order, base_shape + (TILE,), 0, 2 ** 20) * TILE + lax.broadcasted_iota(jnp.int32, base_shape + (TILE,), 5)
    node_ids = jnp.argsort(scores, axis=5)[..., :8].astype(jnp.int32)
    keeping = jax.random.randint(key_keep, base_shape + (8,), 0, 4) > 0
    corner_iota = lax.broadcasted_iota(jnp.int32, base_shape + (8,), 5)
    keeping = keeping | (corner_iota == 0)
    chosen = jnp.where(keeping, node_ids, -1)
    node_range = lax.broadcasted_iota(jnp.int32, base_shape + (8, TILE), 6)
    return (chosen[..., None] == node_range).astype(jnp.int32)


def draw_live_counts(key, part):
    shape_counts = (N_GX, N_GY, N_GZ, NTB)
    drawn = jax.random.randint(jax.random.fold_in(key, 21), shape_counts, 1, CAP // 2 + 1)
    summed = lax.broadcasted_iota(jnp.int32, shape_counts, 0) + lax.broadcasted_iota(jnp.int32, shape_counts, 1) + lax.broadcasted_iota(jnp.int32, shape_counts, 2)
    full_tile = lax.broadcasted_iota(jnp.int32, shape_counts, 3) == summed % NTB
    return jnp.where(full_tile, CAP, drawn).astype(jnp.int32)


def draw_shear_modulus(key, part):
    shape_values = (N_GX, N_GY, N_GZ, NTB, CAP)
    uniform_draw = jax.random.uniform(jax.random.fold_in(key, 31), shape_values, jnp.float32)
    base_values = jnp.exp(jnp.log(0.5) + uniform_draw * (jnp.log(1.5) - jnp.log(0.5)))
    ranking = (lax.broadcasted_iota(jnp.int32, shape_values, 0) * N_GY + lax.broadcasted_iota(jnp.int32, shape_values, 1)) * N_GZ + lax.broadcasted_iota(jnp.int32, shape_values, 2)
    rising = 1.0 + 2.0 * ranking.astype(jnp.float32) / max(N_GX * N_GY * N_GZ - 1, 1)
    return (base_values * rising).astype(jnp.float32)


def levels(stream_key, extent, shards, low, largest):
    loudness, own = 1.0, jax.random.fold_in(stream_key, 6)
    for axis_at, parts in shards:
        heights = jnp.exp(jax.random.uniform(jax.random.fold_in(own, axis_at), (parts,), jnp.float32, low / len(shards), largest / len(shards)))
        loudness = loudness * jnp.repeat(heights, extent[axis_at] // parts).reshape([-1 if axis == axis_at else 1 for axis in range(len(extent))])
    return loudness


def setup_inputs(seed: int = 0) -> dict:
    splits = jax.random.split(jax.random.key(seed), 6)
    return {
        "incidence": draw_incidence(jax.random.fold_in(splits[5], 71), 0),
        "live_counts": draw_live_counts(jax.random.fold_in(splits[5], 71), 0),
        "lame_first": jnp.clip(jnp.exp(math.log(2.0) - 1.3862944 * jax.random.uniform(splits[2], (N_GX, N_GY, N_GZ, NTB, CAP), jnp.float32) ** levels(splits[2], (N_GX, N_GY, N_GZ, NTB, CAP), ((0, 4), (1, 4), (2, 2)), -0.2, 0.2)), 0.5, 2.0),
        "shear_modulus": draw_shear_modulus(jax.random.fold_in(splits[5], 71), 0),
        "stretch": jnp.clip(jnp.exp(math.log(2.0) - 1.3862944 * jax.random.uniform(splits[4], (3, N_GX, N_GY, N_GZ, NTB, CAP), jnp.float32) ** levels(splits[4], (3, N_GX, N_GY, N_GZ, NTB, CAP), ((1, 4), (2, 4), (3, 2)), -0.2, 0.2)), 0.5, 2.0),
    }


def corner_table():
    corner_signs = np.array([[sign_x, sign_y, sign_z] for sign_z in (-1.0, 1.0) for sign_y in (-1.0, 1.0) for sign_x in (-1.0, 1.0)])
    gauss_points = corner_signs / math.sqrt(3.0)
    shape_grads = np.zeros((8, 8, 3))
    for gauss_index in range(8):
        for corner_index in range(8):
            for axis_index in range(3):
                product_value = corner_signs[corner_index, axis_index] / 8.0
                for other_axis in range(3):
                    if other_axis != axis_index:
                        product_value = product_value * (1.0 + corner_signs[corner_index, other_axis] * gauss_points[gauss_index, other_axis])
                shape_grads[gauss_index, corner_index, axis_index] = product_value
    table_values = np.zeros((8, 3, 8, 3))
    for gauss_index in range(8):
        for first_corner in range(8):
            for first_axis in range(3):
                for second_corner in range(8):
                    for second_axis in range(3):
                        table_values[first_corner, first_axis, second_corner, second_axis] += shape_grads[gauss_index, first_corner, first_axis] * shape_grads[gauss_index, second_corner, second_axis]
    return table_values

def element_matrices(first_param, shear_values, lengths):
    inverse = 2.0 / lengths
    scaling = inverse[:, None, :] * inverse[None, :, :]
    volume = lengths[0] * lengths[1] * lengths[2] / 8.0
    ref_table = jnp.asarray(corner_table(), jnp.float32)
    coupled = ref_table[None] * jnp.transpose(scaling, (2, 0, 1))[:, None, :, None, :]
    contracted = coupled[:, :, 0, :, 0] + coupled[:, :, 1, :, 1] + coupled[:, :, 2, :, 2]
    unit_matrix = jnp.eye(3, dtype=jnp.float32)
    matrices = first_param[:, None, None, None, None] * coupled + shear_values[:, None, None, None, None] * (contracted[:, :, None, :, None] * unit_matrix[None, None, :, None, :] + jnp.transpose(coupled, (0, 1, 4, 3, 2)))
    return matrices * volume[:, None, None, None, None]

def assemble_block(matrices, onehot):
    spread = jnp.einsum('epiqj,eqb->epijb', matrices, onehot, precision=lax.Precision.HIGHEST)
    return jnp.einsum('epa,epijb->iajb', onehot, spread, precision=lax.Precision.HIGHEST)

def reference(incidence, live_counts, lame_first, shear_modulus, stretch):
    tile_total = N_GX * N_GY * NTB
    slot_total = N_GZ * CAP
    onehot_all = jnp.transpose(incidence, (0, 1, 3, 2, 4, 5, 6)).reshape(tile_total, slot_total, 8, TILE)
    live_mask = (jnp.arange(CAP, dtype=jnp.int32)[None, None, None, None, :] < live_counts[..., None]).astype(jnp.float32)

    def regroup(values):
        return jnp.transpose(values, (0, 1, 3, 2, 4)).reshape(tile_total, slot_total)
    stretch_all = jnp.transpose(stretch, (1, 2, 4, 3, 5, 0)).reshape(tile_total, slot_total, 3)

    def one_tile(packed):
        onehot, alive_mask, first_param, shear_values, lengths = packed
        matrices = element_matrices(first_param, shear_values, lengths.T) * alive_mask[:, None, None, None, None]
        return assemble_block(matrices, onehot.astype(jnp.float32))
    blocks = lax.map(one_tile, (onehot_all, regroup(live_mask), regroup(lame_first), regroup(shear_modulus), stretch_all))
    flattened = blocks.reshape(tile_total, 3 * TILE, 3 * TILE)
    grand_total = jnp.sum(jnp.trace(flattened, axis1=1, axis2=2))
    mean_diag = grand_total / (3 * TILE * tile_total)
    return (blocks / mean_diag).reshape(N_GX, N_GY, NTB, 3, TILE, 3, TILE)
```

```python
import functools
import math

import jax
import jax.numpy as jnp
from jax import lax
from jax.experimental import pallas as pl
from jax.experimental.pallas import tpu as pltpu
from jax.sharding import PartitionSpec as P

AXES = ("gx", "gy", "gz")
CORNERS = 8
VMEM_LIMIT = 16 * 2**20
ROWS = 8
DIAGONAL = 2.0 / 9.0


def last_contraction(left, right):
    return lax.dot_general(
        left, right, (((1,), (1,)), ((), ())), preferred_element_type=jnp.float32
    )


def spread_lanes(values, cap):
    width = values.shape[1]
    step = cap
    while step < width:
        values = values + pltpu.roll(values, step, axis=1)
        step *= 2
    return values


def encode_kernel(inc_ref, live_ref, lame_ref, shear_ref, stretch_ref, parts_ref, pay_ref):
    tiles, cap, corners, width = inc_ref.shape
    lanes = corners * cap
    row = lax.broadcasted_iota(jnp.int32, (ROWS, width), 0)
    node = lax.broadcasted_iota(jnp.int32, (ROWS, width), 1)
    reader = jnp.where(row == 0, node, (row == 1).astype(jnp.int32))
    reader = reader.astype(jnp.float32).astype(jnp.bfloat16)
    slot = lax.broadcasted_iota(jnp.int32, (1, lanes), 1) % cap
    partial = jnp.zeros((1, lanes), jnp.float32)
    for t in range(tiles):
        onehot = jnp.concatenate([inc_ref[t, :, p, :] for p in range(corners)], axis=0)
        onehot = onehot.astype(jnp.float32).astype(jnp.bfloat16)
        found = last_contraction(reader, onehot)
        here = (found[1:2] > 0.5) & (slot < live_ref[0, t])
        pay_ref[t] = jnp.zeros((ROWS, lanes), jnp.float32)
        pay_ref[t, 1:2, :cap] = lame_ref[t : t + 1]
        pay_ref[t, 2:3, :cap] = shear_ref[t : t + 1]
        for k in range(3):
            pay_ref[t, 3 + k : 4 + k, :cap] = stretch_ref[k, t : t + 1]
        spread = spread_lanes(pay_ref[t], cap)
        lame, shear = spread[1:2], spread[2:3]
        h0, h1, h2 = spread[3:4], spread[4:5], spread[5:6]
        inverse0, inverse1, inverse2 = 2.0 / h0, 2.0 / h1, 2.0 / h2
        squares = inverse0 * inverse0 + inverse1 * inverse1 + inverse2 * inverse2
        volume = h0 * h1 * h2 / 8.0
        weight = volume * (lame + 4.0 * shear) * squares * DIAGONAL
        partial = partial + jnp.where(here, weight, 0.0)
        pay_ref[t] = spread
        pay_ref[t, 0:1] = jnp.where(here, found[0:1], -1.0)
    parts_ref[...] = jnp.broadcast_to(partial, parts_ref.shape)


def walsh(cap, lanes, mask):
    line = lax.broadcasted_iota(jnp.int32, (lanes, lanes), 0)
    column = lax.broadcasted_iota(jnp.int32, (lanes, lanes), 1)
    odd = (column // cap ^ mask) & ~(line // cap)
    odd = (odd ^ odd >> 1 ^ odd >> 2) & 1
    signs = jnp.where(line % cap == column % cap, 1 - 2 * odd, 0)
    return signs.astype(jnp.float32).astype(jnp.bfloat16)


def assemble(sources, cap, width, block_ref):
    lanes = sources[0].shape[1]
    masks = {(0, 1): 3, (0, 2): 5, (1, 2): 6}
    tables = {mask: walsh(cap, lanes, mask) for mask in (0, 3, 5, 6)}
    mode = lax.broadcasted_iota(jnp.int32, (1, lanes), 1) // cap
    bits = [mode >> k & 1 for k in range(3)]
    thirds = [jnp.where(bit == 1, 1.0 / 3.0, 1.0) for bit in bits]
    node = lax.broadcasted_iota(jnp.int32, (width, lanes), 0).astype(jnp.float32)
    high, low, right = {}, {}, {mask: [] for mask in tables}
    for source in sources:
        onehot = (node == source[0:1]).astype(jnp.float32).astype(jnp.bfloat16)
        modes = {
            mask: jnp.dot(onehot, table, preferred_element_type=jnp.float32)
            for mask, table in tables.items()
        }
        for mask in tables:
            right[mask].append(modes[mask].astype(jnp.bfloat16))
        lame, shear = source[1:2], source[2:3]
        lengths = [source[3 + k : 4 + k] for k in range(3)]
        inverse = [2.0 / length for length in lengths]
        scale = lengths[0] * lengths[1] * lengths[2] / 64.0
        squares = []
        for k in range(3):
            others = thirds[(k + 1) % 3] * thirds[(k + 2) % 3]
            squares.append(jnp.where(bits[k] == 1, others, 0.0) * inverse[k] * inverse[k])
        trace = shear * (squares[0] + squares[1] + squares[2])
        for i in range(3):
            for j in range(3):
                if i == j:
                    factor = scale * ((lame + shear) * squares[i] + trace)
                else:
                    material = jnp.where(bits[i] == 1, lame, shear)
                    factor = scale * inverse[i] * inverse[j] * thirds[3 - i - j] * material
                    factor = jnp.where(bits[i] != bits[j], factor, 0.0)
                weighted = modes[0] * factor
                top = weighted.astype(jnp.bfloat16)
                rest = (weighted - top.astype(jnp.float32)).astype(jnp.bfloat16)
                high.setdefault((i, j), []).append(top)
                low.setdefault((i, j), []).append(rest)
    for mask in right:
        right[mask] = jnp.concatenate(right[mask], axis=1)
    for i in range(3):
        for j in range(3):
            other = right[masks[min(i, j), max(i, j)] if i != j else 0]
            block_ref[i, j] = last_contraction(
                jnp.concatenate(high[i, j], axis=1), other
            ) + last_contraction(jnp.concatenate(low[i, j], axis=1), other)


def pair_kernel(cap, own_ref, other_ref, block_ref):
    me = lax.axis_index("gz")
    assemble([own_ref[me], other_ref[me]], cap, block_ref.shape[2], block_ref)


def many_kernel(cap, all_ref, block_ref):
    sources = [all_ref[z] for z in range(all_ref.shape[0])]
    assemble(sources, cap, block_ref.shape[2], block_ref)


def scale_kernel(entries, parts_ref, block_ref, out_ref, scaled, done):
    mean = jnp.sum(parts_ref[...]) / entries
    copies = []
    for i in range(3):
        for j in range(3):
            scaled[i, j] = block_ref[i, j] / mean
            copy = pltpu.make_async_copy(scaled.at[i, j], out_ref.at[i, j], done.at[i, j])
            copy.start()
            copies.append(copy)
    for copy in copies:
        copy.wait()


def on_device(incidence, live_counts, lame_first, shear_modulus, stretch):
    tiles, cap, corners, width = incidence.shape[3:]
    lanes = corners * cap
    devices = math.prod(lax.axis_size(a) for a in AXES)
    depth = lax.axis_size("gz")
    vmem = pl.BlockSpec(memory_space=pltpu.VMEM)
    smem = pl.BlockSpec(memory_space=pltpu.SMEM)
    anywhere = pl.BlockSpec(memory_space=pl.ANY)
    parts, payload = pl.pallas_call(
        encode_kernel,
        out_shape=(
            jax.ShapeDtypeStruct((devices, lanes), jnp.float32),
            jax.ShapeDtypeStruct((tiles, ROWS, lanes), jnp.float32),
        ),
        in_specs=[vmem, smem, vmem, vmem, vmem],
        out_specs=(vmem, vmem),
        compiler_params=pltpu.CompilerParams(vmem_limit_bytes=VMEM_LIMIT),
        name="encode",
    )(
        incidence.reshape(tiles, cap, corners, width),
        live_counts.reshape(1, tiles),
        lame_first.reshape(tiles, cap),
        shear_modulus.reshape(tiles, cap),
        stretch.reshape(3, tiles, cap),
    )
    parts = lax.all_to_all(parts, AXES, 0, 0, tiled=True)
    block_shape = jax.ShapeDtypeStruct((3, 3, width, width), jnp.float32)
    cost = pl.CostEstimate(
        flops=2 * 18 * width * width * lanes * depth, bytes_accessed=10**6, transcendentals=0
    )
    if depth == 2:
        other = lax.ppermute(payload, "gz", [(0, 1), (1, 0)])
        block = pl.pallas_call(
            functools.partial(pair_kernel, cap),
            out_shape=block_shape,
            in_specs=[vmem, vmem],
            out_specs=vmem,
            cost_estimate=cost,
            compiler_params=pltpu.CompilerParams(vmem_limit_bytes=VMEM_LIMIT),
            name="assemble",
        )(payload, other)
    else:
        gathered = lax.all_to_all(payload, "gz", 0, 0, tiled=True)
        block = pl.pallas_call(
            functools.partial(many_kernel, cap),
            out_shape=block_shape,
            in_specs=[vmem],
            out_specs=vmem,
            cost_estimate=cost,
            compiler_params=pltpu.CompilerParams(vmem_limit_bytes=VMEM_LIMIT),
            name="assemble",
        )(gathered)
    entries = 3 * width * lax.axis_size("gx") * lax.axis_size("gy") * tiles
    out = pl.pallas_call(
        functools.partial(scale_kernel, float(entries)),
        out_shape=block_shape,
        in_specs=[vmem, vmem],
        out_specs=anywhere,
        scratch_shapes=[
            pltpu.VMEM((3, 3, width, width), jnp.float32),
            pltpu.SemaphoreType.DMA((3, 3)),
        ],
        compiler_params=pltpu.CompilerParams(vmem_limit_bytes=VMEM_LIMIT),
        name="scale",
    )(parts, block)
    return jnp.transpose(out, (0, 2, 1, 3)).reshape(1, 1, 1, 3, width, 3, width)


def solution(mesh):
    return jax.shard_map(
        on_device,
        mesh=mesh,
        in_specs=(
            P("gx", "gy", "gz", None, None, None, None),
            P("gx", "gy", "gz", None),
            P("gx", "gy", "gz", None, None),
            P("gx", "gy", "gz", None, None),
            P(None, "gx", "gy", "gz", None, None),
        ),
        out_specs=P("gx", "gy", "gz", None, None, None, None),
        check_vma=False,
    )
```

```python
import math

import jax
import jax.numpy as jnp
from jax import lax
from jax.experimental import pallas as pl
from jax.experimental.pallas import tpu as pltpu
from jax.sharding import PartitionSpec as P

AXES = ("gx", "gy", "gz")
VMEM_LIMIT = 16 * 2**20
FIELDS = 8
DIAGONAL = 2.0 / 9.0


def last_contraction(left, right):
    return lax.dot_general(
        left, right, (((1,), (1,)), ((), ())), preferred_element_type=jnp.float32
    )


def whole(space):
    return pl.BlockSpec(memory_space=space)


def encode_kernel(
    targets, inc_hbm, live_hbm, lame_hbm, shear_hbm, stretch_hbm, pay_ref,
    inc_ref, live_ref, params_ref, inc_done, small_done,
):
    tiles, cap, corners, width = inc_ref.shape
    lanes = corners * cap
    small = [
        pltpu.make_async_copy(live_hbm, live_ref, small_done.at[0]),
        pltpu.make_async_copy(lame_hbm, params_ref.at[0], small_done.at[1]),
        pltpu.make_async_copy(shear_hbm, params_ref.at[1], small_done.at[2]),
        pltpu.make_async_copy(stretch_hbm, params_ref.at[2:5], small_done.at[3]),
    ]
    large = [
        pltpu.make_async_copy(inc_hbm.at[t], inc_ref.at[t], inc_done.at[t]) for t in range(tiles)
    ]
    for copy in large + small:
        copy.start()
    row = lax.broadcasted_iota(jnp.int32, (8, width), 0)
    node = lax.broadcasted_iota(jnp.int32, (8, width), 1)
    reader = jnp.where(row == 0, node, (row == 1).astype(jnp.int32))
    reader = reader.astype(jnp.float32).astype(jnp.bfloat16)
    slot = lax.broadcasted_iota(jnp.int32, (1, lanes), 1) % cap
    for copy in small:
        copy.wait()
    lame, shear = params_ref[0], params_ref[1]
    lengths = [params_ref[2 + k] for k in range(3)]
    inverse = [2.0 / length for length in lengths]
    squares = inverse[0] * inverse[0] + inverse[1] * inverse[1] + inverse[2] * inverse[2]
    volume = lengths[0] * lengths[1] * lengths[2] / 8.0
    weight = volume * (lame + 4.0 * shear) * squares * DIAGONAL
    partial = jnp.zeros((1, cap), jnp.float32)
    node_ids = []
    for t in range(tiles):
        large[t].wait()
        onehot = jnp.concatenate([inc_ref[t, :, p, :] for p in range(corners)], axis=0)
        found = last_contraction(reader, onehot.astype(jnp.float32).astype(jnp.bfloat16))
        here = (found[1:2] > 0.5) & (slot < live_ref[:, t : t + 1])
        node_ids.append(jnp.where(here, found[0:1], -1.0))
        count = here.astype(jnp.float32)
        step = lanes
        while step > cap:
            step //= 2
            count = count + pltpu.roll(count, step, axis=1)
        partial = partial + weight[t : t + 1] * count[:, :cap]
    for t in range(tiles):
        fields = [length[t : t + 1] for length in lengths[::-1]]
        fields += [shear[t : t + 1], lame[t : t + 1]]
        unused = jnp.zeros((FIELDS - 1 - len(fields), cap), jnp.float32)
        fields = jnp.concatenate([partial, unused, *fields], axis=0)
        fields = jnp.concatenate([fields, jnp.zeros((FIELDS, lanes - cap), jnp.float32)], axis=1)
        fields = pltpu.roll(fields, 0, axis=1, stride=cap, stride_axis=0)
        fields = jnp.sum(fields, axis=0, keepdims=True)
        both = jnp.concatenate([node_ids[t], fields], axis=0)
        for member, target in enumerate(targets):
            if target == t:
                pay_ref[member] = both


def walsh(cap, lanes, mask):
    line = lax.broadcasted_iota(jnp.int32, (lanes, lanes), 0)
    column = lax.broadcasted_iota(jnp.int32, (lanes, lanes), 1)
    odd = (column // cap ^ mask) & ~(line // cap)
    odd = (odd ^ odd >> 1 ^ odd >> 2) & 1
    signs = jnp.where(line % cap == column % cap, 1 - 2 * odd, 0)
    return signs.astype(jnp.float32).astype(jnp.bfloat16)


def assemble_kernel(depth, cap, place, pay_ref, block_ref):
    width = block_ref.shape[2]
    lanes = pay_ref.shape[2]
    lane = lax.broadcasted_iota(jnp.int32, (1, lanes), 1)
    mode = lane // cap
    bits = [mode >> k & 1 for k in range(3)]
    thirds = [jnp.where(bit == 1, 1.0 / 3.0, 1.0) for bit in bits]
    masks = {(0, 1): 3, (0, 2): 5, (1, 2): 6}
    tables = {mask: walsh(cap, lanes, mask) for mask in (0, 3, 5, 6)}
    node = lax.broadcasted_iota(jnp.int32, (width, lanes), 0).astype(jnp.float32)
    start = place()
    high, low, right = {}, {}, {mask: [] for mask in tables}
    for source in range(depth):
        payload = pay_ref[start + source]
        fields = jnp.broadcast_to(payload[1:2], (FIELDS, lanes))
        fields = pltpu.roll(fields, 0, axis=1, stride=cap, stride_axis=0)
        fields = jnp.where(lane < cap, fields, 0.0)
        step = cap
        while step < lanes:
            fields = fields + pltpu.roll(fields, step, axis=1)
            step *= 2
        lame, shear = fields[1:2], fields[2:3]
        lengths = [fields[3 + k : 4 + k] for k in range(3)]
        onehot = (node == payload[0:1]).astype(jnp.float32).astype(jnp.bfloat16)
        modes = {
            mask: jnp.dot(onehot, table, preferred_element_type=jnp.float32)
            for mask, table in tables.items()
        }
        for mask in tables:
            right[mask].append(modes[mask].astype(jnp.bfloat16))
        inverse = [2.0 / length for length in lengths]
        scale = lengths[0] * lengths[1] * lengths[2] / 64.0
        squares = []
        for k in range(3):
            others = thirds[(k + 1) % 3] * thirds[(k + 2) % 3]
            squares.append(jnp.where(bits[k] == 1, others, 0.0) * inverse[k] * inverse[k])
        trace = shear * (squares[0] + squares[1] + squares[2])
        for i in range(3):
            for j in range(3):
                if i == j:
                    factor = scale * ((lame + shear) * squares[i] + trace)
                else:
                    material = jnp.where(bits[i] == 1, lame, shear)
                    factor = scale * inverse[i] * inverse[j] * thirds[3 - i - j] * material
                    factor = jnp.where(bits[i] != bits[j], factor, 0.0)
                weighted = modes[0] * factor
                top = weighted.astype(jnp.bfloat16)
                rest = (weighted - top.astype(jnp.float32)).astype(jnp.bfloat16)
                high.setdefault((i, j), []).append(top)
                low.setdefault((i, j), []).append(rest)
    for mask in right:
        right[mask] = jnp.concatenate(right[mask], axis=1)
    for i in range(3):
        for j in range(3):
            other = right[masks[min(i, j), max(i, j)] if i != j else 0]
            block_ref[i, j] = last_contraction(
                jnp.concatenate(high[i, j], axis=1), other
            ) + last_contraction(jnp.concatenate(low[i, j], axis=1), other)


def scale_kernel(entries, cap, parts_ref, swapped_ref, block_ref, out_ref, scaled, done):
    mean = jnp.sum((parts_ref[...] + swapped_ref[...])[:, :cap]) / entries
    copies = []
    for i in range(3):
        for j in range(3):
            scaled[i, j] = block_ref[i, j] / mean
            copy = pltpu.make_async_copy(scaled.at[i, j], out_ref.at[i, j], done.at[i, j])
            copy.start()
            copies.append(copy)
    for copy in copies:
        copy.wait()


def call(kernel, name, out_shape, in_specs, out_spec, scratch=(), flops=10**6):
    return pl.pallas_call(
        kernel,
        out_shape=out_shape,
        in_specs=in_specs,
        out_specs=out_spec,
        scratch_shapes=scratch,
        cost_estimate=pl.CostEstimate(flops=flops, bytes_accessed=10**6, transcendentals=0),
        compiler_params=pltpu.CompilerParams(vmem_limit_bytes=VMEM_LIMIT),
        name=name,
    )


def on_device(incidence, live_counts, lame_first, shear_modulus, stretch):
    tiles, cap, corners, width = incidence.shape[3:]
    lanes = corners * cap
    n_gx, n_gy, depth = (lax.axis_size(a) for a in AXES)
    places = range(n_gx * n_gy * depth - 1, -1, -1)
    groups = [[i for i in places if i // (n_gy * depth) % 2 == half] for half in range(2)]
    members = len(groups[0])
    targets = [i % depth for i in groups[0]]

    def place():
        rank = lax.axis_index("gx") // 2 * n_gy + lax.axis_index("gy")
        return members - (rank + 1) * depth

    vmem, hbm = whole(pltpu.VMEM), whole(pltpu.HBM)
    payload = call(
        lambda *refs: encode_kernel(targets, *refs),
        "encode",
        jax.ShapeDtypeStruct((members, 2, lanes), jnp.float32),
        [hbm] * 5,
        vmem,
        [
            pltpu.VMEM((tiles, cap, corners, width), jnp.int32),
            pltpu.VMEM((1, tiles), jnp.int32),
            pltpu.VMEM((5, tiles, cap), jnp.float32),
            pltpu.SemaphoreType.DMA((tiles,)),
            pltpu.SemaphoreType.DMA((4,)),
        ],
    )(
        *(
            pltpu.with_memory_space_constraint(value, pltpu.HBM)
            for value in (
                incidence.reshape(tiles, cap, corners, width),
                live_counts.reshape(1, tiles),
                lame_first.reshape(tiles, cap),
                shear_modulus.reshape(tiles, cap),
                stretch.reshape(3, tiles, cap),
            )
        )
    )
    gathered = lax.all_to_all(payload, AXES, 0, 0, axis_index_groups=groups, tiled=True)
    parts = jnp.sum(gathered[:, 1], axis=0, keepdims=True)
    swapped = lax.ppermute(parts, "gx", [(i, i ^ 1) for i in range(n_gx)])
    block_shape = jax.ShapeDtypeStruct((3, 3, width, width), jnp.float32)
    block = call(
        lambda *refs: assemble_kernel(depth, cap, place, *refs),
        "assemble",
        block_shape,
        [vmem],
        vmem,
        flops=2 * 18 * width * width * lanes * depth,
    )(gathered)
    entries = float(3 * width * n_gx * n_gy * tiles)
    out = call(
        lambda *refs: scale_kernel(entries, cap, *refs),
        "scale",
        block_shape,
        [vmem] * 3,
        hbm,
        [
            pltpu.VMEM((3, 3, width, width), jnp.float32),
            pltpu.SemaphoreType.DMA((3, 3)),
        ],
    )(parts, swapped, block)
    return jnp.transpose(out, (0, 2, 1, 3)).reshape(1, 1, 1, 3, width, 3, width)


def solution(mesh):
    return jax.shard_map(
        on_device,
        mesh=mesh,
        in_specs=(
            P("gx", "gy", "gz", None, None, None, None),
            P("gx", "gy", "gz", None),
            P("gx", "gy", "gz", None, None),
            P("gx", "gy", "gz", None, None),
            P(None, "gx", "gy", "gz", None, None),
        ),
        out_specs=P("gx", "gy", "gz", None, None, None, None),
        check_vma=False,
    )
```

```python
import math

import jax
import jax.numpy as jnp
from jax import lax
from jax.experimental import pallas as pl
from jax.experimental.pallas import tpu as pltpu
from jax.sharding import PartitionSpec as P

AXES = ("gx", "gy", "gz")
VMEM_LIMIT = 16 * 2**20
CHUNKS = 2
FIELDS = 8
DIAGONAL = 2.0 / 9.0


def last_contraction(left, right):
    return lax.dot_general(
        left, right, (((1,), (1,)), ((), ())), preferred_element_type=jnp.float32
    )


def whole(space):
    return pl.BlockSpec(memory_space=space)


def encode_kernel(
    targets, inc_hbm, live_hbm, lame_hbm, shear_hbm, stretch_hbm, pay_ref,
    inc_ref, live_ref, params_ref, inc_done, small_done,
):
    tiles, cap, corners, width = inc_ref.shape
    lanes = corners * cap
    chunks = inc_done.shape[1]
    part = cap // chunks
    small = [
        pltpu.make_async_copy(live_hbm, live_ref, small_done.at[0]),
        pltpu.make_async_copy(lame_hbm, params_ref.at[0], small_done.at[1]),
        pltpu.make_async_copy(shear_hbm, params_ref.at[1], small_done.at[2]),
        pltpu.make_async_copy(stretch_hbm, params_ref.at[2:5], small_done.at[3]),
    ]
    large = []
    for t in range(tiles):
        for c in range(chunks):
            slots = pl.ds(c * part, part)
            large.append(
                pltpu.make_async_copy(inc_hbm.at[t, slots], inc_ref.at[t, slots], inc_done.at[t, c])
            )
    for copy in small + large:
        copy.start()
    row = lax.broadcasted_iota(jnp.int32, (8, width), 0)
    node = lax.broadcasted_iota(jnp.int32, (8, width), 1)
    reader = jnp.where(row == 0, node, (row == 1).astype(jnp.int32))
    reader = reader.astype(jnp.float32).astype(jnp.bfloat16)
    lane = lax.broadcasted_iota(jnp.int32, (1, lanes), 1)
    line = lax.broadcasted_iota(jnp.int32, (cap, lanes), 0)
    spread = (line == lax.broadcasted_iota(jnp.int32, (cap, lanes), 1) // corners).astype(jnp.float32)
    for copy in small:
        copy.wait()
    lame, shear = params_ref[0], params_ref[1]
    lengths = [params_ref[2 + k] for k in range(3)]
    inverse = [2.0 / length for length in lengths]
    squares = inverse[0] * inverse[0] + inverse[1] * inverse[1] + inverse[2] * inverse[2]
    volume = lengths[0] * lengths[1] * lengths[2] / 8.0
    weight = volume * (lame + 4.0 * shear) * squares * DIAGONAL
    weight = jnp.dot(
        weight, spread, preferred_element_type=jnp.float32, precision=lax.Precision.HIGHEST
    )
    field_rows = []
    for t in range(tiles):
        fields = [length[t : t + 1] for length in lengths[::-1]]
        fields += [shear[t : t + 1], lame[t : t + 1]]
        unused = jnp.zeros((FIELDS - len(fields), cap), jnp.float32)
        fields = jnp.concatenate([unused, *fields], axis=0)
        fields = jnp.concatenate([fields, jnp.zeros((FIELDS, lanes - cap), jnp.float32)], axis=1)
        fields = pltpu.roll(fields, 0, axis=1, stride=cap, stride_axis=0)
        field_rows.append(jnp.sum(fields, axis=0, keepdims=True))
    live = [lane // corners < live_ref[:, t : t + 1] for t in range(tiles)]
    for copy in large:
        copy.wait()
    partial = jnp.zeros((1, lanes), jnp.float32)
    node_ids = []
    onehot = inc_ref[...].reshape(tiles * lanes, width)
    found = last_contraction(reader, onehot.astype(jnp.float32).astype(jnp.bfloat16))
    for t in range(tiles):
        position = found[0:1, t * lanes : (t + 1) * lanes]
        here = (found[1:2, t * lanes : (t + 1) * lanes] > 0.5) & live[t]
        node_ids.append(jnp.where(here, position, -1.0))
        partial = partial + jnp.where(here, weight[t : t + 1], 0.0)
    partial = jnp.sum(partial, axis=1, keepdims=True)
    for t in range(tiles):
        both = jnp.concatenate(
            [node_ids[t], jnp.where(lane == 0, partial, field_rows[t])], axis=0
        )
        for member, target in enumerate(targets):
            if target == t:
                pay_ref[member] = both


def walsh(cap, lanes, mask):
    corners = lanes // cap
    line = lax.broadcasted_iota(jnp.int32, (lanes, lanes), 0)
    column = lax.broadcasted_iota(jnp.int32, (lanes, lanes), 1)
    odd = (column // cap ^ mask) & ~(line % corners)
    odd = (odd ^ odd >> 1 ^ odd >> 2) & 1
    signs = jnp.where(line // corners == column % cap, 1 - 2 * odd, 0)
    return signs.astype(jnp.float32).astype(jnp.bfloat16)


def assemble_kernel(depth, cap, place, pay_ref, block_ref):
    width = block_ref.shape[2]
    lanes = pay_ref.shape[2]
    lane = lax.broadcasted_iota(jnp.int32, (1, lanes), 1)
    mode = lane // cap
    bits = [mode >> k & 1 for k in range(3)]
    thirds = [jnp.where(bit == 1, 1.0 / 3.0, 1.0) for bit in bits]
    masks = {(0, 1): 3, (0, 2): 5, (1, 2): 6}
    tables = {mask: walsh(cap, lanes, mask) for mask in (0, 3, 5, 6)}
    node = lax.broadcasted_iota(jnp.int32, (width, lanes), 0).astype(jnp.float32)
    start = place()
    high, low, right = {}, {}, {mask: [] for mask in tables}
    for source in range(depth):
        payload = pay_ref[start + source]
        fields = jnp.broadcast_to(payload[1:2], (FIELDS, lanes))
        fields = pltpu.roll(fields, 0, axis=1, stride=cap, stride_axis=0)
        fields = jnp.where(lane < cap, fields, 0.0)
        step = cap
        while step < lanes:
            fields = fields + pltpu.roll(fields, step, axis=1)
            step *= 2
        lame, shear = fields[1:2], fields[2:3]
        lengths = [fields[3 + k : 4 + k] for k in range(3)]
        onehot = (node == payload[0:1]).astype(jnp.float32).astype(jnp.bfloat16)
        modes = {
            mask: jnp.dot(onehot, table, preferred_element_type=jnp.float32)
            for mask, table in tables.items()
        }
        for mask in tables:
            right[mask].append(modes[mask].astype(jnp.bfloat16))
        inverse = [2.0 / length for length in lengths]
        scale = lengths[0] * lengths[1] * lengths[2] / 64.0
        squares = []
        for k in range(3):
            others = thirds[(k + 1) % 3] * thirds[(k + 2) % 3]
            squares.append(jnp.where(bits[k] == 1, others, 0.0) * inverse[k] * inverse[k])
        trace = shear * (squares[0] + squares[1] + squares[2])
        for i in range(3):
            for j in range(3):
                if i == j:
                    factor = scale * ((lame + shear) * squares[i] + trace)
                else:
                    material = jnp.where(bits[i] == 1, lame, shear)
                    factor = scale * inverse[i] * inverse[j] * thirds[3 - i - j] * material
                    factor = jnp.where(bits[i] != bits[j], factor, 0.0)
                weighted = modes[0] * factor
                top = weighted.astype(jnp.bfloat16)
                rest = (weighted - top.astype(jnp.float32)).astype(jnp.bfloat16)
                high.setdefault((i, j), []).append(top)
                low.setdefault((i, j), []).append(rest)
    for mask in right:
        right[mask] = jnp.concatenate(right[mask], axis=1)
    for i in range(3):
        for j in range(3):
            other = right[masks[min(i, j), max(i, j)] if i != j else 0]
            block_ref[i, j] = last_contraction(
                jnp.concatenate(high[i, j], axis=1), other
            ) + last_contraction(jnp.concatenate(low[i, j], axis=1), other)


def scale_kernel(entries, parts_ref, swapped_ref, block_ref, out_ref, scaled, done):
    mean = (parts_ref[...] + swapped_ref[...])[:, :1] / entries
    inverse = 1.0 / mean
    copies = []
    for i in range(3):
        for j in range(3):
            scaled[i, j] = block_ref[i, j] * inverse
            copy = pltpu.make_async_copy(scaled.at[i, j], out_ref.at[i, j], done.at[i, j])
            copy.start()
            copies.append(copy)
    for copy in copies:
        copy.wait()


def call(kernel, name, out_shape, in_specs, out_spec, scratch=(), flops=10**6):
    return pl.pallas_call(
        kernel,
        out_shape=out_shape,
        in_specs=in_specs,
        out_specs=out_spec,
        scratch_shapes=scratch,
        cost_estimate=pl.CostEstimate(flops=flops, bytes_accessed=10**6, transcendentals=0),
        compiler_params=pltpu.CompilerParams(vmem_limit_bytes=VMEM_LIMIT),
        name=name,
    )


def on_device(incidence, live_counts, lame_first, shear_modulus, stretch):
    tiles, cap, corners, width = incidence.shape[3:]
    lanes = corners * cap
    n_gx, n_gy, depth = (lax.axis_size(a) for a in AXES)
    places = range(n_gx * n_gy * depth - 1, -1, -1)
    groups = [[i for i in places if i // (n_gy * depth) % 2 == half] for half in range(2)]
    members = len(groups[0])
    targets = [i % depth for i in groups[0]]

    def place():
        rank = lax.axis_index("gx") // 2 * n_gy + lax.axis_index("gy")
        return members - (rank + 1) * depth

    vmem, hbm = whole(pltpu.VMEM), whole(pltpu.HBM)
    payload = call(
        lambda *refs: encode_kernel(targets, *refs),
        "encode",
        jax.ShapeDtypeStruct((members, 2, lanes), jnp.float32),
        [hbm] * 5,
        vmem,
        [
            pltpu.VMEM((tiles, cap, corners, width), jnp.int32),
            pltpu.VMEM((1, tiles), jnp.int32),
            pltpu.VMEM((5, tiles, cap), jnp.float32),
            pltpu.SemaphoreType.DMA((tiles, CHUNKS)),
            pltpu.SemaphoreType.DMA((4,)),
        ],
    )(
        *(
            pltpu.with_memory_space_constraint(value, pltpu.HBM)
            for value in (
                incidence.reshape(tiles, cap, corners, width),
                live_counts.reshape(1, tiles),
                lame_first.reshape(tiles, cap),
                shear_modulus.reshape(tiles, cap),
                stretch.reshape(3, tiles, cap),
            )
        )
    )
    gathered = lax.all_to_all(payload, AXES, 0, 0, axis_index_groups=groups, tiled=True)
    parts = jnp.sum(gathered[:, 1], axis=0, keepdims=True)
    swapped = lax.ppermute(parts, "gx", [(i, i ^ 1) for i in range(n_gx)])
    block_shape = jax.ShapeDtypeStruct((3, 3, width, width), jnp.float32)
    block = call(
        lambda *refs: assemble_kernel(depth, cap, place, *refs),
        "assemble",
        block_shape,
        [vmem],
        vmem,
        flops=2 * 18 * width * width * lanes * depth,
    )(gathered)
    entries = float(3 * width * n_gx * n_gy * tiles)
    out = call(
        lambda *refs: scale_kernel(entries, *refs),
        "scale",
        block_shape,
        [vmem] * 3,
        hbm,
        [
            pltpu.VMEM((3, 3, width, width), jnp.float32),
            pltpu.SemaphoreType.DMA((3, 3)),
        ],
    )(parts, swapped, block)
    return jnp.transpose(out, (0, 2, 1, 3)).reshape(1, 1, 1, 3, width, 3, width)


def solution(mesh):
    return jax.shard_map(
        on_device,
        mesh=mesh,
        in_specs=(
            P("gx", "gy", "gz", None, None, None, None),
            P("gx", "gy", "gz", None),
            P("gx", "gy", "gz", None, None),
            P("gx", "gy", "gz", None, None),
            P(None, "gx", "gy", "gz", None, None),
        ),
        out_specs=P("gx", "gy", "gz", None, None, None, None),
        check_vma=False,
    )
```

```python
import math

import jax
import jax.numpy as jnp
from jax import lax
from jax.experimental import pallas as pl
from jax.experimental.pallas import tpu as pltpu
from jax.sharding import PartitionSpec as P

AXES = ("gx", "gy", "gz")
VMEM_LIMIT = 16 * 2**20
CUTS = (0, 3, 6, 9)
FIELDS = 8
DIAGONAL = 2.0 / 9.0


def last_contraction(left, right):
    return lax.dot_general(
        left, right, (((1,), (1,)), ((), ())), preferred_element_type=jnp.float32
    )


def whole(space):
    return pl.BlockSpec(memory_space=space)


def encode_kernel(
    targets, inc_hbm, live_hbm, lame_hbm, shear_hbm, stretch_hbm, pay_ref,
    inc_ref, live_ref, params_ref, inc_done, small_done,
):
    tiles, cap, corners, width = inc_ref.shape
    lanes = corners * cap
    small = [
        pltpu.make_async_copy(live_hbm, live_ref, small_done.at[0]),
        pltpu.make_async_copy(lame_hbm, params_ref.at[0], small_done.at[1]),
        pltpu.make_async_copy(shear_hbm, params_ref.at[1], small_done.at[2]),
        pltpu.make_async_copy(stretch_hbm, params_ref.at[2:5], small_done.at[3]),
    ]
    large = pltpu.make_async_copy(inc_hbm, inc_ref, inc_done)
    for copy in [large, *small]:
        copy.start()
    row = lax.broadcasted_iota(jnp.int32, (8, width), 0)
    node = lax.broadcasted_iota(jnp.int32, (8, width), 1)
    reader = jnp.where(row == 0, node, (row == 1).astype(jnp.int32))
    reader = reader.astype(jnp.float32).astype(jnp.bfloat16)
    lane = lax.broadcasted_iota(jnp.int32, (1, lanes), 1)
    line = lax.broadcasted_iota(jnp.int32, (cap, lanes), 0)
    spread = (line == lax.broadcasted_iota(jnp.int32, (cap, lanes), 1) // corners).astype(jnp.float32)
    for copy in small:
        copy.wait()
    lame, shear = params_ref[0], params_ref[1]
    lengths = [params_ref[2 + k] for k in range(3)]
    inverse = [2.0 / length for length in lengths]
    squares = inverse[0] * inverse[0] + inverse[1] * inverse[1] + inverse[2] * inverse[2]
    volume = lengths[0] * lengths[1] * lengths[2] / 8.0
    weight = volume * (lame + 4.0 * shear) * squares * DIAGONAL
    weight = jnp.dot(
        weight, spread, preferred_element_type=jnp.float32, precision=lax.Precision.HIGHEST
    )
    field_rows = []
    for t in range(tiles):
        fields = [length[t : t + 1] for length in lengths[::-1]]
        fields += [shear[t : t + 1], lame[t : t + 1]]
        unused = jnp.zeros((FIELDS - len(fields), cap), jnp.float32)
        fields = jnp.concatenate([unused, *fields], axis=0)
        fields = jnp.concatenate([fields, jnp.zeros((FIELDS, lanes - cap), jnp.float32)], axis=1)
        fields = pltpu.roll(fields, 0, axis=1, stride=cap, stride_axis=0)
        field_rows.append(jnp.sum(fields, axis=0, keepdims=True))
    live = [lane // corners < live_ref[:, t : t + 1] for t in range(tiles)]
    large.wait()
    partial = jnp.zeros((1, lanes), jnp.float32)
    node_ids = []
    onehot = inc_ref[...].reshape(tiles * lanes, width)
    found = last_contraction(reader, onehot.astype(jnp.float32).astype(jnp.bfloat16))
    for t in range(tiles):
        position = found[0:1, t * lanes : (t + 1) * lanes]
        here = (found[1:2, t * lanes : (t + 1) * lanes] > 0.5) & live[t]
        node_ids.append(jnp.where(here, position, -1.0))
        partial = partial + jnp.where(here, weight[t : t + 1], 0.0)
    partial = jnp.sum(partial, axis=1, keepdims=True)
    for t in range(tiles):
        both = jnp.concatenate(
            [node_ids[t], jnp.where(lane == 0, partial, field_rows[t])], axis=0
        )
        for member, target in enumerate(targets):
            if target == t:
                pay_ref[member] = both


def walsh(cap, lanes, mask):
    corners = lanes // cap
    line = lax.broadcasted_iota(jnp.int32, (lanes, lanes), 0)
    column = lax.broadcasted_iota(jnp.int32, (lanes, lanes), 1)
    odd = (column // cap ^ mask) & ~(line % corners)
    odd = (odd ^ odd >> 1 ^ odd >> 2) & 1
    signs = jnp.where(line // corners == column % cap, 1 - 2 * odd, 0)
    return signs.astype(jnp.float32).astype(jnp.bfloat16)


def assemble_kernel(depth, cap, place, pay_ref, block_ref):
    width = block_ref.shape[1]
    lanes = pay_ref.shape[2]
    lane = lax.broadcasted_iota(jnp.int32, (1, lanes), 1)
    mode = lane // cap
    bits = [mode >> k & 1 for k in range(3)]
    thirds = [jnp.where(bit == 1, 1.0 / 3.0, 1.0) for bit in bits]
    masks = {(0, 1): 3, (0, 2): 5, (1, 2): 6}
    tables = {mask: walsh(cap, lanes, mask) for mask in (0, 3, 5, 6)}
    node = lax.broadcasted_iota(jnp.int32, (width, lanes), 0).astype(jnp.float32)
    start = place()
    high, low, right = {}, {}, {mask: [] for mask in tables}
    for source in range(depth):
        payload = pay_ref[start + source]
        fields = jnp.broadcast_to(payload[1:2], (FIELDS, lanes))
        fields = pltpu.roll(fields, 0, axis=1, stride=cap, stride_axis=0)
        fields = jnp.where(lane < cap, fields, 0.0)
        step = cap
        while step < lanes:
            fields = fields + pltpu.roll(fields, step, axis=1)
            step *= 2
        lame, shear = fields[1:2], fields[2:3]
        lengths = [fields[3 + k : 4 + k] for k in range(3)]
        onehot = (node == payload[0:1]).astype(jnp.float32).astype(jnp.bfloat16)
        modes = {
            mask: jnp.dot(onehot, table, preferred_element_type=jnp.float32)
            for mask, table in tables.items()
        }
        for mask in tables:
            right[mask].append(modes[mask].astype(jnp.bfloat16))
        inverse = [2.0 / length for length in lengths]
        scale = lengths[0] * lengths[1] * lengths[2] / 64.0
        squares = []
        for k in range(3):
            others = thirds[(k + 1) % 3] * thirds[(k + 2) % 3]
            squares.append(jnp.where(bits[k] == 1, others, 0.0) * inverse[k] * inverse[k])
        trace = shear * (squares[0] + squares[1] + squares[2])
        for i in range(3):
            for j in range(3):
                if i == j:
                    factor = scale * ((lame + shear) * squares[i] + trace)
                else:
                    material = jnp.where(bits[i] == 1, lame, shear)
                    factor = scale * inverse[i] * inverse[j] * thirds[3 - i - j] * material
                    factor = jnp.where(bits[i] != bits[j], factor, 0.0)
                weighted = modes[0] * factor
                top = weighted.astype(jnp.bfloat16)
                rest = (weighted - top.astype(jnp.float32)).astype(jnp.bfloat16)
                high.setdefault((i, j), []).append(top)
                low.setdefault((i, j), []).append(rest)
    for mask in right:
        right[mask] = jnp.concatenate(right[mask], axis=1)
    for i in range(3):
        for j in range(3):
            other = right[masks[min(i, j), max(i, j)] if i != j else 0]
            block_ref[3 * i + j] = last_contraction(
                jnp.concatenate(high[i, j], axis=1), other
            ) + last_contraction(jnp.concatenate(low[i, j], axis=1), other)


def scale_kernel(entries, parts_ref, swapped_ref, block_ref, out_ref, scaled, done):
    mean = (parts_ref[...] + swapped_ref[...])[:, :1] / entries
    inverse = 1.0 / mean
    copies = []
    for n, (first, last) in enumerate(zip(CUTS[:-1], CUTS[1:])):
        part = pl.ds(first, last - first)
        scaled[part] = block_ref[part] * inverse
        copy = pltpu.make_async_copy(scaled.at[part], out_ref.at[part], done.at[n])
        copy.start()
        copies.append(copy)
    for copy in copies:
        copy.wait()


def call(kernel, name, out_shape, in_specs, out_spec, scratch=(), flops=10**6):
    return pl.pallas_call(
        kernel,
        out_shape=out_shape,
        in_specs=in_specs,
        out_specs=out_spec,
        scratch_shapes=scratch,
        cost_estimate=pl.CostEstimate(flops=flops, bytes_accessed=10**6, transcendentals=0),
        compiler_params=pltpu.CompilerParams(vmem_limit_bytes=VMEM_LIMIT),
        name=name,
    )


def on_device(incidence, live_counts, lame_first, shear_modulus, stretch):
    tiles, cap, corners, width = incidence.shape[3:]
    lanes = corners * cap
    n_gx, n_gy, depth = (lax.axis_size(a) for a in AXES)
    places = range(n_gx * n_gy * depth - 1, -1, -1)
    turn = [(g ^ g >> 1) & 1 for g in range(n_gx)]
    groups = [[i for i in places if turn[i // (n_gy * depth)] == half] for half in range(2)]
    members = len(groups[0])
    targets = [i % depth for i in groups[0]]

    def place():
        rank = lax.axis_index("gx") // 2 * n_gy + lax.axis_index("gy")
        return members - (rank + 1) * depth

    vmem, hbm = whole(pltpu.VMEM), whole(pltpu.HBM)
    payload = call(
        lambda *refs: encode_kernel(targets, *refs),
        "encode",
        jax.ShapeDtypeStruct((members, 2, lanes), jnp.float32),
        [hbm] * 5,
        vmem,
        [
            pltpu.VMEM((tiles, cap, corners, width), jnp.int32),
            pltpu.VMEM((1, tiles), jnp.int32),
            pltpu.VMEM((5, tiles, cap), jnp.float32),
            pltpu.SemaphoreType.DMA,
            pltpu.SemaphoreType.DMA((4,)),
        ],
    )(
        *(
            pltpu.with_memory_space_constraint(value, pltpu.HBM)
            for value in (
                incidence.reshape(tiles, cap, corners, width),
                live_counts.reshape(1, tiles),
                lame_first.reshape(tiles, cap),
                shear_modulus.reshape(tiles, cap),
                stretch.reshape(3, tiles, cap),
            )
        )
    )
    gathered = lax.all_to_all(payload, AXES, 0, 0, axis_index_groups=groups, tiled=True)
    parts = jnp.sum(gathered[:, 1], axis=0, keepdims=True)
    swapped = lax.ppermute(parts, "gx", [(i, i ^ 1) for i in range(n_gx)])
    block_shape = jax.ShapeDtypeStruct((9, width, width), jnp.float32)
    block = call(
        lambda *refs: assemble_kernel(depth, cap, place, *refs),
        "assemble",
        block_shape,
        [vmem],
        vmem,
        flops=2 * 18 * width * width * lanes * depth,
    )(gathered)
    entries = float(3 * width * n_gx * n_gy * tiles)
    out = call(
        lambda *refs: scale_kernel(entries, *refs),
        "scale",
        block_shape,
        [vmem] * 3,
        hbm,
        [
            pltpu.VMEM((9, width, width), jnp.float32),
            pltpu.SemaphoreType.DMA((len(CUTS) - 1,)),
        ],
    )(parts, swapped, block)
    out = jnp.transpose(out.reshape(3, 3, width, width), (0, 2, 1, 3))
    return out.reshape(1, 1, 1, 3, width, 3, width)


def solution(mesh):
    return jax.shard_map(
        on_device,
        mesh=mesh,
        in_specs=(
            P("gx", "gy", "gz", None, None, None, None),
            P("gx", "gy", "gz", None),
            P("gx", "gy", "gz", None, None),
            P("gx", "gy", "gz", None, None),
            P(None, "gx", "gy", "gz", None, None),
        ),
        out_specs=P("gx", "gy", "gz", None, None, None, None),
        check_vma=False,
    )
```

```python
import math

import jax
import jax.numpy as jnp
from jax import lax
from jax.experimental import pallas as pl
from jax.experimental.pallas import tpu as pltpu
from jax.sharding import PartitionSpec as P

AXES = ("gx", "gy", "gz")
VMEM_LIMIT = 16 * 2**20
CUTS = (0, 3, 6, 9)
FIELDS = 8
DIAGONAL = 2.0 / 9.0


def last_contraction(left, right):
    return lax.dot_general(
        left, right, (((1,), (1,)), ((), ())), preferred_element_type=jnp.float32
    )


def whole(space):
    return pl.BlockSpec(memory_space=space)


def encode_kernel(
    targets, inc_hbm, live_hbm, lame_hbm, shear_hbm, stretch_hbm, pay_ref,
    inc_ref, live_ref, params_ref, inc_done, small_done,
):
    tiles, cap, corners, width = inc_ref.shape
    lanes = corners * cap
    small = [
        pltpu.make_async_copy(live_hbm, live_ref, small_done.at[0]),
        pltpu.make_async_copy(lame_hbm, params_ref.at[0], small_done.at[1]),
        pltpu.make_async_copy(shear_hbm, params_ref.at[1], small_done.at[2]),
        pltpu.make_async_copy(stretch_hbm, params_ref.at[2:5], small_done.at[3]),
    ]
    large = pltpu.make_async_copy(inc_hbm, inc_ref, inc_done)
    part = cap // 2
    pieces = [
        pltpu.make_async_copy(inc_hbm.at[t, pl.ds(c, part)], inc_ref.at[t, pl.ds(c, part)], inc_done)
        for t in range(tiles)
        for c in (0, part)
    ]
    for copy in [*pieces[:2], *small, *pieces[2:]]:
        copy.start()
    row = lax.broadcasted_iota(jnp.int32, (8, width), 0)
    node = lax.broadcasted_iota(jnp.int32, (8, width), 1)
    reader = jnp.where(row == 0, node, (row == 1).astype(jnp.int32))
    reader = reader.astype(jnp.float32).astype(jnp.bfloat16)
    lane = lax.broadcasted_iota(jnp.int32, (1, lanes), 1)
    line = lax.broadcasted_iota(jnp.int32, (cap, lanes), 0)
    spread = (line == lax.broadcasted_iota(jnp.int32, (cap, lanes), 1) // corners).astype(jnp.float32)
    for copy in small:
        copy.wait()
    lame, shear = params_ref[0], params_ref[1]
    lengths = [params_ref[2 + k] for k in range(3)]
    inverse = [2.0 / length for length in lengths]
    squares = inverse[0] * inverse[0] + inverse[1] * inverse[1] + inverse[2] * inverse[2]
    volume = lengths[0] * lengths[1] * lengths[2] / 8.0
    weight = volume * (lame + 4.0 * shear) * squares * DIAGONAL
    weight = jnp.dot(
        weight, spread, preferred_element_type=jnp.float32, precision=lax.Precision.HIGHEST
    )
    field_rows = []
    for t in range(tiles):
        fields = [length[t : t + 1] for length in lengths[::-1]]
        fields += [shear[t : t + 1], lame[t : t + 1]]
        unused = jnp.zeros((FIELDS - len(fields), cap), jnp.float32)
        fields = jnp.concatenate([unused, *fields], axis=0)
        fields = jnp.concatenate([fields, jnp.zeros((FIELDS, lanes - cap), jnp.float32)], axis=1)
        fields = pltpu.roll(fields, 0, axis=1, stride=cap, stride_axis=0)
        field_rows.append(jnp.sum(fields, axis=0, keepdims=True))
    live = [lane // corners < live_ref[:, t : t + 1] for t in range(tiles)]
    large.wait()
    partial = jnp.zeros((1, lanes), jnp.float32)
    node_ids = []
    onehot = inc_ref[...].reshape(tiles * lanes, width)
    found = last_contraction(reader, onehot.astype(jnp.float32).astype(jnp.bfloat16))
    for t in range(tiles):
        position = found[0:1, t * lanes : (t + 1) * lanes]
        here = (found[1:2, t * lanes : (t + 1) * lanes] > 0.5) & live[t]
        node_ids.append(jnp.where(here, position, -1.0))
        partial = partial + jnp.where(here, weight[t : t + 1], 0.0)
    partial = jnp.sum(partial, axis=1, keepdims=True)
    for t in range(tiles):
        both = jnp.concatenate(
            [node_ids[t], jnp.where(lane == 0, partial, field_rows[t])], axis=0
        )
        for member, target in enumerate(targets):
            if target == t:
                pay_ref[member] = both


def walsh(cap, lanes, mask):
    corners = lanes // cap
    line = lax.broadcasted_iota(jnp.int32, (lanes, lanes), 0)
    column = lax.broadcasted_iota(jnp.int32, (lanes, lanes), 1)
    odd = (column // cap ^ mask) & ~(line % corners)
    odd = (odd ^ odd >> 1 ^ odd >> 2) & 1
    signs = jnp.where(line // corners == column % cap, 1 - 2 * odd, 0)
    return signs.astype(jnp.float32).astype(jnp.bfloat16)


def assemble_kernel(depth, cap, place, pay_ref, block_ref):
    width = block_ref.shape[1]
    lanes = pay_ref.shape[2]
    lane = lax.broadcasted_iota(jnp.int32, (1, lanes), 1)
    mode = lane // cap
    bits = [mode >> k & 1 for k in range(3)]
    thirds = [jnp.where(bit == 1, 1.0 / 3.0, 1.0) for bit in bits]
    masks = {(0, 1): 3, (0, 2): 5, (1, 2): 6}
    tables = {mask: walsh(cap, lanes, mask) for mask in (0, 3, 5, 6)}
    node = lax.broadcasted_iota(jnp.int32, (width, lanes), 0).astype(jnp.float32)
    start = place()
    high, low, right = {}, {}, {mask: [] for mask in tables}
    for source in range(depth):
        payload = pay_ref[start + source]
        fields = jnp.broadcast_to(payload[1:2], (FIELDS, lanes))
        fields = pltpu.roll(fields, 0, axis=1, stride=cap, stride_axis=0)
        fields = jnp.where(lane < cap, fields, 0.0)
        step = cap
        while step < lanes:
            fields = fields + pltpu.roll(fields, step, axis=1)
            step *= 2
        lame, shear = fields[1:2], fields[2:3]
        lengths = [fields[3 + k : 4 + k] for k in range(3)]
        onehot = (node == payload[0:1]).astype(jnp.float32).astype(jnp.bfloat16)
        modes = {
            mask: jnp.dot(onehot, table, preferred_element_type=jnp.float32)
            for mask, table in tables.items()
        }
        for mask in tables:
            right[mask].append(modes[mask].astype(jnp.bfloat16))
        inverse = [2.0 / length for length in lengths]
        scale = lengths[0] * lengths[1] * lengths[2] / 64.0
        squares = []
        for k in range(3):
            others = thirds[(k + 1) % 3] * thirds[(k + 2) % 3]
            squares.append(jnp.where(bits[k] == 1, others, 0.0) * inverse[k] * inverse[k])
        trace = shear * (squares[0] + squares[1] + squares[2])
        for i in range(3):
            for j in range(3):
                if i == j:
                    factor = scale * ((lame + shear) * squares[i] + trace)
                else:
                    material = jnp.where(bits[i] == 1, lame, shear)
                    factor = scale * inverse[i] * inverse[j] * thirds[3 - i - j] * material
                    factor = jnp.where(bits[i] != bits[j], factor, 0.0)
                weighted = modes[0] * factor
                top = weighted.astype(jnp.bfloat16)
                rest = (weighted - top.astype(jnp.float32)).astype(jnp.bfloat16)
                high.setdefault((i, j), []).append(top)
                low.setdefault((i, j), []).append(rest)
    for mask in right:
        right[mask] = jnp.concatenate(right[mask], axis=1)
    for i in range(3):
        for j in range(3):
            other = right[masks[min(i, j), max(i, j)] if i != j else 0]
            block_ref[3 * i + j] = last_contraction(
                jnp.concatenate(high[i, j], axis=1), other
            ) + last_contraction(jnp.concatenate(low[i, j], axis=1), other)


def scale_kernel(entries, parts_ref, swapped_ref, block_ref, out_ref, scaled, done):
    mean = (parts_ref[...] + swapped_ref[...])[:, :1] / entries
    inverse = 1.0 / mean
    copies = []
    for n, (first, last) in enumerate(zip(CUTS[:-1], CUTS[1:])):
        part = pl.ds(first, last - first)
        scaled[part] = block_ref[part] * inverse
        copy = pltpu.make_async_copy(scaled.at[part], out_ref.at[part], done.at[n])
        copy.start()
        copies.append(copy)
    for copy in copies:
        copy.wait()


def call(kernel, name, out_shape, in_specs, out_spec, scratch=(), flops=10**6):
    return pl.pallas_call(
        kernel,
        out_shape=out_shape,
        in_specs=in_specs,
        out_specs=out_spec,
        scratch_shapes=scratch,
        cost_estimate=pl.CostEstimate(flops=flops, bytes_accessed=10**6, transcendentals=0),
        compiler_params=pltpu.CompilerParams(vmem_limit_bytes=VMEM_LIMIT),
        name=name,
    )


def on_device(incidence, live_counts, lame_first, shear_modulus, stretch):
    tiles, cap, corners, width = incidence.shape[3:]
    lanes = corners * cap
    n_gx, n_gy, depth = (lax.axis_size(a) for a in AXES)
    places = [
        (2 * k + int(k + h > (n_gx // 2 + n_gy) // 2 - 1), h, z)
        for k in reversed(range(n_gx // 2))
        for h in reversed(range(n_gy))
        for z in reversed(range(depth))
    ]
    groups = [[((g ^ half) * n_gy + h) * depth + z for g, h, z in places] for half in range(2)]
    members = len(groups[0])
    targets = [i % depth for i in groups[0]]

    def place():
        rank = lax.axis_index("gx") // 2 * n_gy + lax.axis_index("gy")
        return members - (rank + 1) * depth

    vmem, hbm = whole(pltpu.VMEM), whole(pltpu.HBM)
    payload = call(
        lambda *refs: encode_kernel(targets, *refs),
        "encode",
        jax.ShapeDtypeStruct((members, 2, lanes), jnp.float32),
        [hbm] * 5,
        vmem,
        [
            pltpu.VMEM((tiles, cap, corners, width), jnp.int32),
            pltpu.VMEM((1, tiles), jnp.int32),
            pltpu.VMEM((5, tiles, cap), jnp.float32),
            pltpu.SemaphoreType.DMA,
            pltpu.SemaphoreType.DMA((4,)),
        ],
    )(
        *(
            pltpu.with_memory_space_constraint(value, pltpu.HBM)
            for value in (
                incidence.reshape(tiles, cap, corners, width),
                live_counts.reshape(1, tiles),
                lame_first.reshape(tiles, cap),
                shear_modulus.reshape(tiles, cap),
                stretch.reshape(3, tiles, cap),
            )
        )
    )
    gathered = lax.all_to_all(payload, AXES, 0, 0, axis_index_groups=groups, tiled=True)
    parts = jnp.sum(gathered[:, 1], axis=0, keepdims=True)
    swapped = lax.ppermute(parts, "gx", [(i, i ^ 1) for i in range(n_gx)])
    block_shape = jax.ShapeDtypeStruct((9, width, width), jnp.float32)
    block = call(
        lambda *refs: assemble_kernel(depth, cap, place, *refs),
        "assemble",
        block_shape,
        [vmem],
        vmem,
        flops=2 * 18 * width * width * lanes * depth,
    )(gathered)
    entries = float(3 * width * n_gx * n_gy * tiles)
    out = call(
        lambda *refs: scale_kernel(entries, *refs),
        "scale",
        block_shape,
        [vmem] * 3,
        hbm,
        [
            pltpu.VMEM((9, width, width), jnp.float32),
            pltpu.SemaphoreType.DMA((len(CUTS) - 1,)),
        ],
    )(parts, swapped, block)
    out = jnp.transpose(out.reshape(3, 3, width, width), (0, 2, 1, 3))
    return out.reshape(1, 1, 1, 3, width, 3, width)


def solution(mesh):
    return jax.shard_map(
        on_device,
        mesh=mesh,
        in_specs=(
            P("gx", "gy", "gz", None, None, None, None),
            P("gx", "gy", "gz", None),
            P("gx", "gy", "gz", None, None),
            P("gx", "gy", "gz", None, None),
            P(None, "gx", "gy", "gz", None, None),
        ),
        out_specs=P("gx", "gy", "gz", None, None, None, None),
        check_vma=False,
    )
```

```python
import math

import jax
import jax.numpy as jnp
from jax import lax
from jax.experimental import pallas as pl
from jax.experimental.pallas import tpu as pltpu
from jax.sharding import PartitionSpec as P

AXES = ("gx", "gy", "gz")
VMEM_LIMIT = 16 * 2**20
CUTS = (0, 2, 5, 9)
FIELDS = 8
DIAGONAL = 2.0 / 9.0


def last_contraction(left, right):
    return lax.dot_general(
        left, right, (((1,), (1,)), ((), ())), preferred_element_type=jnp.float32
    )


def whole(space):
    return pl.BlockSpec(memory_space=space)


def encode_kernel(
    targets, inc_hbm, live_hbm, lame_hbm, shear_hbm, stretch_hbm, pay_ref,
    inc_ref, live_ref, params_ref, inc_done, small_done,
):
    tiles, cap, corners, width = inc_ref.shape
    lanes = corners * cap
    small = [
        pltpu.make_async_copy(live_hbm, live_ref, small_done.at[0]),
        pltpu.make_async_copy(lame_hbm, params_ref.at[0], small_done.at[1]),
        pltpu.make_async_copy(shear_hbm, params_ref.at[1], small_done.at[2]),
        pltpu.make_async_copy(stretch_hbm, params_ref.at[2:5], small_done.at[3]),
    ]
    large = pltpu.make_async_copy(inc_hbm, inc_ref, inc_done)
    part = cap // 2
    pieces = [
        pltpu.make_async_copy(inc_hbm.at[t, pl.ds(c, part)], inc_ref.at[t, pl.ds(c, part)], inc_done)
        for t in range(tiles)
        for c in (0, part)
    ]
    for copy in [*pieces[:2], *small, *pieces[2:]]:
        copy.start()
    row = lax.broadcasted_iota(jnp.int32, (8, width), 0)
    node = lax.broadcasted_iota(jnp.int32, (8, width), 1)
    reader = jnp.where(row == 0, node, (row == 1).astype(jnp.int32))
    reader = reader.astype(jnp.float32).astype(jnp.bfloat16)
    lane = lax.broadcasted_iota(jnp.int32, (1, lanes), 1)
    line = lax.broadcasted_iota(jnp.int32, (cap, lanes), 0)
    spread = (line == lax.broadcasted_iota(jnp.int32, (cap, lanes), 1) // corners).astype(jnp.float32)
    for copy in small:
        copy.wait()
    lame, shear = params_ref[0], params_ref[1]
    lengths = [params_ref[2 + k] for k in range(3)]
    inverse = [2.0 / length for length in lengths]
    squares = inverse[0] * inverse[0] + inverse[1] * inverse[1] + inverse[2] * inverse[2]
    volume = lengths[0] * lengths[1] * lengths[2] / 8.0
    weight = volume * (lame + 4.0 * shear) * squares * DIAGONAL
    weight = jnp.dot(
        weight, spread, preferred_element_type=jnp.float32, precision=lax.Precision.HIGHEST
    )
    field_rows = []
    for t in range(tiles):
        fields = [length[t : t + 1] for length in lengths[::-1]]
        fields += [shear[t : t + 1], lame[t : t + 1]]
        unused = jnp.zeros((FIELDS - len(fields), cap), jnp.float32)
        fields = jnp.concatenate([unused, *fields], axis=0)
        fields = jnp.concatenate([fields, jnp.zeros((FIELDS, lanes - cap), jnp.float32)], axis=1)
        fields = pltpu.roll(fields, 0, axis=1, stride=cap, stride_axis=0)
        field_rows.append(jnp.sum(fields, axis=0, keepdims=True))
    live = [lane // corners < live_ref[:, t : t + 1] for t in range(tiles)]
    large.wait()
    partial = jnp.zeros((1, lanes), jnp.float32)
    node_ids = []
    onehot = inc_ref[...].reshape(tiles * lanes, width)
    found = last_contraction(reader, onehot.astype(jnp.float32).astype(jnp.bfloat16))
    for t in range(tiles):
        position = found[0:1, t * lanes : (t + 1) * lanes]
        here = (found[1:2, t * lanes : (t + 1) * lanes] > 0.5) & live[t]
        node_ids.append(jnp.where(here, position, -1.0))
        partial = partial + jnp.where(here, weight[t : t + 1], 0.0)
    partial = jnp.sum(partial, axis=1, keepdims=True)
    for t in range(tiles):
        both = jnp.concatenate(
            [node_ids[t], jnp.where(lane == 0, partial, field_rows[t])], axis=0
        )
        for member, target in enumerate(targets):
            if target == t:
                pay_ref[member] = both


def walsh(cap, lanes, mask):
    corners = lanes // cap
    line = lax.broadcasted_iota(jnp.int32, (lanes, lanes), 0)
    column = lax.broadcasted_iota(jnp.int32, (lanes, lanes), 1)
    odd = (column // cap ^ mask) & ~(line % corners)
    odd = (odd ^ odd >> 1 ^ odd >> 2) & 1
    signs = jnp.where(line // corners == column % cap, 1 - 2 * odd, 0)
    return signs.astype(jnp.float32).astype(jnp.bfloat16)


def assemble_kernel(depth, cap, place, pay_ref, block_ref):
    width = block_ref.shape[1]
    lanes = pay_ref.shape[2]
    lane = lax.broadcasted_iota(jnp.int32, (1, lanes), 1)
    mode = lane // cap
    bits = [mode >> k & 1 for k in range(3)]
    thirds = [jnp.where(bit == 1, 1.0 / 3.0, 1.0) for bit in bits]
    masks = {(0, 1): 3, (0, 2): 5, (1, 2): 6}
    tables = {mask: walsh(cap, lanes, mask) for mask in (0, 3, 5, 6)}
    node = lax.broadcasted_iota(jnp.int32, (width, lanes), 0).astype(jnp.float32)
    start = place()
    high, low, right = {}, {}, {mask: [] for mask in tables}
    for source in range(depth):
        payload = pay_ref[start + source]
        fields = jnp.broadcast_to(payload[1:2], (FIELDS, lanes))
        fields = pltpu.roll(fields, 0, axis=1, stride=cap, stride_axis=0)
        fields = jnp.where(lane < cap, fields, 0.0)
        step = cap
        while step < lanes:
            fields = fields + pltpu.roll(fields, step, axis=1)
            step *= 2
        lame, shear = fields[1:2], fields[2:3]
        lengths = [fields[3 + k : 4 + k] for k in range(3)]
        onehot = (node == payload[0:1]).astype(jnp.float32).astype(jnp.bfloat16)
        modes = {
            mask: jnp.dot(onehot, table, preferred_element_type=jnp.float32)
            for mask, table in tables.items()
        }
        for mask in tables:
            right[mask].append(modes[mask].astype(jnp.bfloat16))
        inverse = [2.0 / length for length in lengths]
        scale = lengths[0] * lengths[1] * lengths[2] / 64.0
        squares = []
        for k in range(3):
            others = thirds[(k + 1) % 3] * thirds[(k + 2) % 3]
            squares.append(jnp.where(bits[k] == 1, others, 0.0) * inverse[k] * inverse[k])
        trace = shear * (squares[0] + squares[1] + squares[2])
        for i in range(3):
            for j in range(3):
                if i == j:
                    factor = scale * ((lame + shear) * squares[i] + trace)
                else:
                    material = jnp.where(bits[i] == 1, lame, shear)
                    factor = scale * inverse[i] * inverse[j] * thirds[3 - i - j] * material
                    factor = jnp.where(bits[i] != bits[j], factor, 0.0)
                weighted = modes[0] * factor
                top = weighted.astype(jnp.bfloat16)
                rest = (weighted - top.astype(jnp.float32)).astype(jnp.bfloat16)
                high.setdefault((i, j), []).append(top)
                low.setdefault((i, j), []).append(rest)
    for mask in right:
        right[mask] = jnp.concatenate(right[mask], axis=1)
    for i in range(3):
        for j in range(3):
            other = right[masks[min(i, j), max(i, j)] if i != j else 0]
            block_ref[3 * i + j] = last_contraction(
                jnp.concatenate(high[i, j], axis=1), other
            ) + last_contraction(jnp.concatenate(low[i, j], axis=1), other)


def scale_kernel(entries, parts_ref, swapped_ref, block_ref, out_ref, scaled, done):
    mean = (parts_ref[...] + swapped_ref[...])[:, :1] / entries
    inverse = 1.0 / mean
    copies = []
    for n, (first, last) in enumerate(zip(CUTS[:-1], CUTS[1:])):
        part = pl.ds(first, last - first)
        scaled[part] = block_ref[part] * inverse
        copy = pltpu.make_async_copy(scaled.at[part], out_ref.at[part], done.at[n])
        copy.start()
        copies.append(copy)
    for copy in copies:
        copy.wait()


def call(kernel, name, out_shape, in_specs, out_spec, scratch=(), flops=10**6):
    return pl.pallas_call(
        kernel,
        out_shape=out_shape,
        in_specs=in_specs,
        out_specs=out_spec,
        scratch_shapes=scratch,
        cost_estimate=pl.CostEstimate(flops=flops, bytes_accessed=10**6, transcendentals=0),
        compiler_params=pltpu.CompilerParams(vmem_limit_bytes=VMEM_LIMIT),
        name=name,
    )


def on_device(incidence, live_counts, lame_first, shear_modulus, stretch):
    tiles, cap, corners, width = incidence.shape[3:]
    lanes = corners * cap
    n_gx, n_gy, depth = (lax.axis_size(a) for a in AXES)
    places = [
        (2 * k + int(k + h > (n_gx // 2 + n_gy) // 2 - 1), h, z)
        for k in reversed(range(n_gx // 2))
        for h in reversed(range(n_gy))
        for z in reversed(range(depth))
    ]
    groups = [[((g ^ half) * n_gy + h) * depth + z for g, h, z in places] for half in range(2)]
    members = len(groups[0])
    targets = [i % depth for i in groups[0]]

    def place():
        rank = lax.axis_index("gx") // 2 * n_gy + lax.axis_index("gy")
        return members - (rank + 1) * depth

    vmem, hbm = whole(pltpu.VMEM), whole(pltpu.HBM)
    payload = call(
        lambda *refs: encode_kernel(targets, *refs),
        "encode",
        jax.ShapeDtypeStruct((members, 2, lanes), jnp.float32),
        [hbm] * 5,
        vmem,
        [
            pltpu.VMEM((tiles, cap, corners, width), jnp.int32),
            pltpu.VMEM((1, tiles), jnp.int32),
            pltpu.VMEM((5, tiles, cap), jnp.float32),
            pltpu.SemaphoreType.DMA,
            pltpu.SemaphoreType.DMA((4,)),
        ],
    )(
        *(
            pltpu.with_memory_space_constraint(value, pltpu.HBM)
            for value in (
                incidence.reshape(tiles, cap, corners, width),
                live_counts.reshape(1, tiles),
                lame_first.reshape(tiles, cap),
                shear_modulus.reshape(tiles, cap),
                stretch.reshape(3, tiles, cap),
            )
        )
    )
    gathered = lax.all_to_all(payload, AXES, 0, 0, axis_index_groups=groups, tiled=True)
    parts = jnp.sum(gathered[:, 1], axis=0, keepdims=True)
    swapped = lax.ppermute(parts, "gx", [(i, i ^ 1) for i in range(n_gx)])
    block_shape = jax.ShapeDtypeStruct((9, width, width), jnp.float32)
    block = call(
        lambda *refs: assemble_kernel(depth, cap, place, *refs),
        "assemble",
        block_shape,
        [vmem],
        vmem,
        flops=2 * 18 * width * width * lanes * depth,
    )(gathered)
    entries = float(3 * width * n_gx * n_gy * tiles)
    out = call(
        lambda *refs: scale_kernel(entries, *refs),
        "scale",
        block_shape,
        [vmem] * 3,
        hbm,
        [
            pltpu.VMEM((9, width, width), jnp.float32),
            pltpu.SemaphoreType.DMA((len(CUTS) - 1,)),
        ],
    )(parts, swapped, block)
    out = jnp.transpose(out.reshape(3, 3, width, width), (0, 2, 1, 3))
    return out.reshape(1, 1, 1, 3, width, 3, width)


def solution(mesh):
    return jax.shard_map(
        on_device,
        mesh=mesh,
        in_specs=(
            P("gx", "gy", "gz", None, None, None, None),
            P("gx", "gy", "gz", None),
            P("gx", "gy", "gz", None, None),
            P("gx", "gy", "gz", None, None),
            P(None, "gx", "gy", "gz", None, None),
        ),
        out_specs=P("gx", "gy", "gz", None, None, None, None),
        check_vma=False,
    )
```

```python
import math

import jax
import jax.numpy as jnp
from jax import lax
from jax.experimental import pallas as pl
from jax.experimental.pallas import tpu as pltpu
from jax.sharding import PartitionSpec as P

AXES = ("gx", "gy", "gz")
VMEM_LIMIT = 16 * 2**20
CUTS = (0, 2, 5, 9)
FIELDS = 8
DIAGONAL = 2.0 / 9.0


def last_contraction(left, right):
    return lax.dot_general(
        left, right, (((1,), (1,)), ((), ())), preferred_element_type=jnp.float32
    )


def whole(space):
    return pl.BlockSpec(memory_space=space)


def encode_kernel(
    targets, inc_hbm, live_hbm, lame_hbm, shear_hbm, stretch_hbm, pay_ref,
    inc_ref, live_ref, params_ref, inc_done, small_done,
):
    tiles, cap, corners, width = inc_ref.shape
    lanes = corners * cap
    small = [
        pltpu.make_async_copy(live_hbm, live_ref, small_done.at[0]),
        pltpu.make_async_copy(lame_hbm, params_ref.at[0], small_done.at[1]),
        pltpu.make_async_copy(shear_hbm, params_ref.at[1], small_done.at[2]),
        pltpu.make_async_copy(stretch_hbm, params_ref.at[2:5], small_done.at[3]),
    ]
    large = pltpu.make_async_copy(inc_hbm, inc_ref, inc_done)
    part = cap // 2
    pieces = [
        pltpu.make_async_copy(inc_hbm.at[t, pl.ds(c, part)], inc_ref.at[t, pl.ds(c, part)], inc_done)
        for t in range(tiles)
        for c in (0, part)
    ]
    for copy in [*pieces[:2], *small, *pieces[2:]]:
        copy.start()
    row = lax.broadcasted_iota(jnp.int32, (8, width), 0)
    node = lax.broadcasted_iota(jnp.int32, (8, width), 1)
    reader = jnp.where(row == 0, node, (row == 1).astype(jnp.int32))
    reader = reader.astype(jnp.float32).astype(jnp.bfloat16)
    lane = lax.broadcasted_iota(jnp.int32, (1, lanes), 1)
    line = lax.broadcasted_iota(jnp.int32, (cap, lanes), 0)
    spread = (line == lax.broadcasted_iota(jnp.int32, (cap, lanes), 1) // corners).astype(jnp.float32)
    for copy in small:
        copy.wait()
    large.wait()
    live = [lane // corners < live_ref[:, t : t + 1] for t in range(tiles)]
    partial = jnp.zeros((1, lanes), jnp.float32)
    node_ids = []
    onehot = inc_ref[...].reshape(tiles * lanes, width)
    found = last_contraction(reader, onehot.astype(jnp.float32).astype(jnp.bfloat16))
    lame, shear = params_ref[0], params_ref[1]
    lengths = [params_ref[2 + k] for k in range(3)]
    inverse = [2.0 / length for length in lengths]
    squares = inverse[0] * inverse[0] + inverse[1] * inverse[1] + inverse[2] * inverse[2]
    volume = lengths[0] * lengths[1] * lengths[2] / 8.0
    weight = volume * (lame + 4.0 * shear) * squares * DIAGONAL
    weight = jnp.dot(
        weight, spread, preferred_element_type=jnp.float32, precision=lax.Precision.HIGHEST
    )
    field_rows = []
    for t in range(tiles):
        fields = [length[t : t + 1] for length in lengths[::-1]]
        fields += [shear[t : t + 1], lame[t : t + 1]]
        unused = jnp.zeros((FIELDS - len(fields), cap), jnp.float32)
        fields = jnp.concatenate([unused, *fields], axis=0)
        fields = jnp.concatenate([fields, jnp.zeros((FIELDS, lanes - cap), jnp.float32)], axis=1)
        fields = pltpu.roll(fields, 0, axis=1, stride=cap, stride_axis=0)
        field_rows.append(jnp.sum(fields, axis=0, keepdims=True))
    for t in range(tiles):
        position = found[0:1, t * lanes : (t + 1) * lanes]
        here = (found[1:2, t * lanes : (t + 1) * lanes] > 0.5) & live[t]
        node_ids.append(jnp.where(here, position, -1.0))
        partial = partial + jnp.where(here, weight[t : t + 1], 0.0)
    partial = jnp.sum(partial, axis=1, keepdims=True)
    for t in range(tiles):
        both = jnp.concatenate(
            [node_ids[t], jnp.where(lane == 0, partial, field_rows[t])], axis=0
        )
        for member, target in enumerate(targets):
            if target == t:
                pay_ref[member] = both


def walsh(cap, lanes, mask):
    corners = lanes // cap
    line = lax.broadcasted_iota(jnp.int32, (lanes, lanes), 0)
    column = lax.broadcasted_iota(jnp.int32, (lanes, lanes), 1)
    odd = (column // cap ^ mask) & ~(line % corners)
    odd = (odd ^ odd >> 1 ^ odd >> 2) & 1
    signs = jnp.where(line // corners == column % cap, 1 - 2 * odd, 0)
    return signs.astype(jnp.float32).astype(jnp.bfloat16)


def assemble_kernel(depth, cap, place, pay_ref, block_ref):
    width = block_ref.shape[1]
    lanes = pay_ref.shape[2]
    lane = lax.broadcasted_iota(jnp.int32, (1, lanes), 1)
    mode = lane // cap
    bits = [mode >> k & 1 for k in range(3)]
    thirds = [jnp.where(bit == 1, 1.0 / 3.0, 1.0) for bit in bits]
    masks = {(0, 1): 3, (0, 2): 5, (1, 2): 6}
    tables = {mask: walsh(cap, lanes, mask) for mask in (0, 3, 5, 6)}
    node = lax.broadcasted_iota(jnp.int32, (width, lanes), 0).astype(jnp.float32)
    start = place()
    high, low, right = {}, {}, {mask: [] for mask in tables}
    for source in range(depth):
        payload = pay_ref[start + source]
        fields = jnp.broadcast_to(payload[1:2], (FIELDS, lanes))
        fields = pltpu.roll(fields, 0, axis=1, stride=cap, stride_axis=0)
        fields = jnp.where(lane < cap, fields, 0.0)
        step = cap
        while step < lanes:
            fields = fields + pltpu.roll(fields, step, axis=1)
            step *= 2
        lame, shear = fields[1:2], fields[2:3]
        lengths = [fields[3 + k : 4 + k] for k in range(3)]
        onehot = (node == payload[0:1]).astype(jnp.float32).astype(jnp.bfloat16)
        modes = {
            mask: jnp.dot(onehot, table, preferred_element_type=jnp.float32)
            for mask, table in tables.items()
        }
        for mask in tables:
            right[mask].append(modes[mask].astype(jnp.bfloat16))
        inverse = [2.0 / length for length in lengths]
        scale = lengths[0] * lengths[1] * lengths[2] / 64.0
        squares = []
        for k in range(3):
            others = thirds[(k + 1) % 3] * thirds[(k + 2) % 3]
            squares.append(jnp.where(bits[k] == 1, others, 0.0) * inverse[k] * inverse[k])
        trace = shear * (squares[0] + squares[1] + squares[2])
        for i in range(3):
            for j in range(3):
                if i == j:
                    factor = scale * ((lame + shear) * squares[i] + trace)
                else:
                    material = jnp.where(bits[i] == 1, lame, shear)
                    factor = scale * inverse[i] * inverse[j] * thirds[3 - i - j] * material
                    factor = jnp.where(bits[i] != bits[j], factor, 0.0)
                weighted = modes[0] * factor
                top = weighted.astype(jnp.bfloat16)
                rest = (weighted - top.astype(jnp.float32)).astype(jnp.bfloat16)
                high.setdefault((i, j), []).append(top)
                low.setdefault((i, j), []).append(rest)
    for mask in right:
        right[mask] = jnp.concatenate(right[mask], axis=1)
    for i in range(3):
        for j in range(3):
            other = right[masks[min(i, j), max(i, j)] if i != j else 0]
            block_ref[3 * i + j] = last_contraction(
                jnp.concatenate(high[i, j], axis=1), other
            ) + last_contraction(jnp.concatenate(low[i, j], axis=1), other)


def scale_kernel(entries, parts_ref, swapped_ref, block_ref, out_ref, scaled, done):
    mean = (parts_ref[...] + swapped_ref[...])[:, :1] / entries
    inverse = 1.0 / mean
    copies = []
    for n, (first, last) in enumerate(zip(CUTS[:-1], CUTS[1:])):
        part = pl.ds(first, last - first)
        scaled[part] = block_ref[part] * inverse
        copy = pltpu.make_async_copy(scaled.at[part], out_ref.at[part], done.at[n])
        copy.start()
        copies.append(copy)
    for copy in copies:
        copy.wait()


def call(kernel, name, out_shape, in_specs, out_spec, scratch=(), flops=10**6):
    return pl.pallas_call(
        kernel,
        out_shape=out_shape,
        in_specs=in_specs,
        out_specs=out_spec,
        scratch_shapes=scratch,
        cost_estimate=pl.CostEstimate(flops=flops, bytes_accessed=10**6, transcendentals=0),
        compiler_params=pltpu.CompilerParams(vmem_limit_bytes=VMEM_LIMIT),
        name=name,
    )


def on_device(incidence, live_counts, lame_first, shear_modulus, stretch):
    tiles, cap, corners, width = incidence.shape[3:]
    lanes = corners * cap
    n_gx, n_gy, depth = (lax.axis_size(a) for a in AXES)
    places = [
        (2 * k + int(k + h > (n_gx // 2 + n_gy) // 2 - 1), h, z)
        for k in reversed(range(n_gx // 2))
        for h in reversed(range(n_gy))
        for z in reversed(range(depth))
    ]
    groups = [[((g ^ half) * n_gy + h) * depth + z for g, h, z in places] for half in range(2)]
    members = len(groups[0])
    targets = [i % depth for i in groups[0]]

    def place():
        rank = lax.axis_index("gx") // 2 * n_gy + lax.axis_index("gy")
        return members - (rank + 1) * depth

    vmem, hbm = whole(pltpu.VMEM), whole(pltpu.HBM)
    payload = call(
        lambda *refs: encode_kernel(targets, *refs),
        "encode",
        jax.ShapeDtypeStruct((members, 2, lanes), jnp.float32),
        [hbm] * 5,
        vmem,
        [
            pltpu.VMEM((tiles, cap, corners, width), jnp.int32),
            pltpu.VMEM((1, tiles), jnp.int32),
            pltpu.VMEM((5, tiles, cap), jnp.float32),
            pltpu.SemaphoreType.DMA,
            pltpu.SemaphoreType.DMA((4,)),
        ],
    )(
        *(
            pltpu.with_memory_space_constraint(value, pltpu.HBM)
            for value in (
                incidence.reshape(tiles, cap, corners, width),
                live_counts.reshape(1, tiles),
                lame_first.reshape(tiles, cap),
                shear_modulus.reshape(tiles, cap),
                stretch.reshape(3, tiles, cap),
            )
        )
    )
    gathered = lax.all_to_all(payload, AXES, 0, 0, axis_index_groups=groups, tiled=True)
    parts = jnp.sum(gathered[:, 1], axis=0, keepdims=True)
    swapped = lax.ppermute(parts, "gx", [(i, i ^ 1) for i in range(n_gx)])
    block_shape = jax.ShapeDtypeStruct((9, width, width), jnp.float32)
    block = call(
        lambda *refs: assemble_kernel(depth, cap, place, *refs),
        "assemble",
        block_shape,
        [vmem],
        vmem,
        flops=2 * 18 * width * width * lanes * depth,
    )(gathered)
    entries = float(3 * width * n_gx * n_gy * tiles)
    out = call(
        lambda *refs: scale_kernel(entries, *refs),
        "scale",
        block_shape,
        [vmem] * 3,
        hbm,
        [
            pltpu.VMEM((9, width, width), jnp.float32),
            pltpu.SemaphoreType.DMA((len(CUTS) - 1,)),
        ],
    )(parts, swapped, block)
    out = jnp.transpose(out.reshape(3, 3, width, width), (0, 2, 1, 3))
    return out.reshape(1, 1, 1, 3, width, 3, width)


def solution(mesh):
    return jax.shard_map(
        on_device,
        mesh=mesh,
        in_specs=(
            P("gx", "gy", "gz", None, None, None, None),
            P("gx", "gy", "gz", None),
            P("gx", "gy", "gz", None, None),
            P("gx", "gy", "gz", None, None),
            P(None, "gx", "gy", "gz", None, None),
        ),
        out_specs=P("gx", "gy", "gz", None, None, None, None),
        check_vma=False,
    )
```
